16 devices in a mesh: dp: 2 (over y, z), tp: 8 (over x, core).
Axes of the slice: x: 4, y: 2, z: 1, core: 2. Of those that a mesh axis runs over, the one named last changes fastest.
The devices are a block of a 4x4x4 slice.
Arguments:
- x: bfloat16 [128, 3584], P('dp'), parts along dimension 0
- k_cache: bfloat16 [128, 4096, 8, 256], P('dp', None, 'tp'), parts along dimension 0
- v_cache: bfloat16 [128, 4096, 8, 256], P('dp', None, 'tp'), parts along dimension 0
- gain_a: bfloat16 [3584], replicated
- wq: bfloat16 [3584, 4096], P(None, 'tp')
- wo: bfloat16 [4096, 3584], P('tp')
- gain_m: bfloat16 [3584], replicated
- w_gate: bfloat16 [3584, 14336], P(None, 'tp')
- w_up: bfloat16 [3584, 14336], P(None, 'tp')
- w_down: bfloat16 [14336, 3584], P('tp')
Outputs:
- output: bfloat16 [128, 3584], P('dp'), parts along dimension 0
There are 2 independent parts. The reference program is written for one: setup_inputs(seed, part) draws one part's arguments, and reference() takes and returns one part's arrays. A program takes and returns all parts, laid end to end along the dimension named above; an argument that names none is the same for every part.
All inputs are finite; a program needn't handle non-finite values.
Results may differ from the reference program's by a relative error of at most 0.017.
Values are sent between devices in bfloat16 or wider.
A program may use at most 1.5 GiB of HBM per device.

```python
import jax
import jax.numpy as jnp
from jax import lax

BATCH = 64
CACHE = 4096
D = 3584
HEADS = 16
KV_HEADS = 8
HEAD = 256
FF = 14336
THETA = 10000


def setup_inputs(seed: int = 0, part: int = 0) -> dict:
    kx, kc, kw, kn, kq, ko, km, kg, ku, kd = jax.random.split(jax.random.key(seed), 10)
    kx, kc, kw = (jax.random.fold_in(k, part) for k in (kx, kc, kw))

    def weights(key, rows, columns):
        return jax.random.normal(key, (rows, columns), jnp.float32) * rows**-0.5

    drawn = {
        "x": jax.random.normal(kx, (BATCH, D), jnp.float32),
        "k_cache": 2 * jax.random.normal(kc, (BATCH, CACHE, KV_HEADS, HEAD), jnp.float32),
        "v_cache": 4 * jax.random.normal(kw, (BATCH, CACHE, KV_HEADS, HEAD), jnp.float32),
        "gain_a": 1 + 0.1 * jax.random.normal(kn, (D,), jnp.float32),
        "wq": 2 * weights(kq, D, HEADS * HEAD),
        "wo": weights(ko, HEADS * HEAD, D),
        "gain_m": 1 + 0.1 * jax.random.normal(km, (D,), jnp.float32),
        "w_gate": weights(kg, D, FF),
        "w_up": weights(ku, D, FF),
        "w_down": 2 * weights(kd, FF, D),
    }
    return {k: v.astype(jnp.bfloat16) for k, v in drawn.items()}


def normed(x, gain):
    wide = x.astype(jnp.float32)
    scale = lax.rsqrt(jnp.mean(wide * wide, -1, keepdims=True) + 1e-6)
    return (wide * scale * gain.astype(jnp.float32)).astype(jnp.bfloat16)


def turned(t, place, theta):
    half = t.shape[-1] // 2
    angle = place.astype(jnp.float32)[:, None] * theta ** (-jnp.arange(half, dtype=jnp.float32) / half)
    cos, sin = jnp.cos(angle)[:, None], jnp.sin(angle)[:, None]
    a, b = t[..., :half].astype(jnp.float32), t[..., half:].astype(jnp.float32)
    return jnp.concatenate([a * cos - b * sin, b * cos + a * sin], -1).astype(jnp.bfloat16)


def matmul(a, w):
    return jnp.dot(a, w, preferred_element_type=jnp.float32).astype(jnp.bfloat16)


def einsum(form, a, b):
    return jnp.einsum(form, a.astype(jnp.float32), b.astype(jnp.float32))


def seen_by(a, wq, k_cache, v_cache, head, theta):
    batch, cache, kv_heads = k_cache.shape[:3]
    place = jnp.full((batch,), cache - 1)
    q = turned(matmul(a, wq).reshape(batch, -1, head), place, theta).reshape(batch, kv_heads, -1, head)
    scores = einsum("bgsd,bugd->bgsu", q, k_cache) * head**-0.5
    weights = jax.nn.softmax(scores, -1).astype(jnp.bfloat16)
    return einsum("bgsu,bugd->bgsd", weights, v_cache).astype(jnp.bfloat16).reshape(batch, -1)


def hidden_of(b, w_gate, w_up):
    gate = jnp.dot(b, w_gate, preferred_element_type=jnp.float32)
    up = jnp.dot(b, w_up, preferred_element_type=jnp.float32)
    return (jax.nn.silu(gate) * up).astype(jnp.bfloat16)


def reference(x, k_cache, v_cache, gain_a, wq, wo, gain_m, w_gate, w_up, w_down):
    seen = seen_by(normed(x, gain_a), wq, k_cache, v_cache, HEAD, THETA)
    h = (x.astype(jnp.float32) + jnp.dot(seen, wo, preferred_element_type=jnp.float32)).astype(jnp.bfloat16)
    hidden = hidden_of(normed(h, gain_m), w_gate, w_up)
    return (h.astype(jnp.float32) + jnp.dot(hidden, w_down, preferred_element_type=jnp.float32)).astype(jnp.bfloat16)
```

```python
import functools

import jax
import jax.numpy as jnp
from jax import lax
from jax.experimental import pallas as pl
from jax.experimental.pallas import tpu as pltpu
from jax.sharding import PartitionSpec as P

HEAD = 256
THETA = 10000
SLOTS = 3
SPLIT = 2
HIDDEN_TILE = 256
OUT_TILE = 512
VMEM_LIMIT = 67_043_328
F32 = jnp.float32
BF16 = jnp.bfloat16


def rem(a, b):
    return a % b if isinstance(a, int) else lax.rem(a, b)


def tile_at(i, size):
    return pl.ds(i * size if isinstance(i, int) else pl.multiple_of(i * size, size), size)


def normed(wide, gain):
    scale = lax.rsqrt(jnp.mean(wide * wide, -1, keepdims=True) + 1e-6)
    return wide * scale * gain


def layer(
    n,
    x_ref, k_ref, v_ref, ga_ref, wq_ref, wo_ref, gm_ref, wg_ref, wu_ref, wd_ref, cs_ref,
    y_ref,
    xv, gav, gmv, csv, ks, vs, wov, wgv, wuv, wdv, qf, scores, seen, terms, hf, bf, b16, hid, outf, out16, sums, yown,
    in_sem, k_sem, v_sem, wq_sem, wo_sem, g_sem, u_sem, d_sem,
    t_send, t_recv, s_send, s_recv, y_send, y_recv, own_sem,
):
    me = lax.axis_index("tp")
    rows, d = xv.shape
    cache, head = ks.shape[1:]
    heads = wq_ref.shape[1] // head
    half = head // 2
    block = terms.shape[2]
    ng, nd = wgv.shape[0], wdv.shape[0]
    gt, dt = wgv.shape[2], wdv.shape[2]

    def peer(j):
        return rem(me + j, n)

    def at(dev):
        return {"tp": dev}

    def kv_start(hbm, slots, sem, s, slot):
        part = cache // SPLIT
        for i in range(SPLIT):
            pltpu.make_async_copy(hbm.at[s, pl.ds(i * part, part)], slots.at[slot, pl.ds(i * part, part)], sem.at[slot]).start()

    def kv_wait(hbm, slots, sem, slot):
        pltpu.make_async_copy(hbm.at[0], slots.at[slot], sem.at[slot]).wait()

    def start_k(s):
        kv_start(k_ref, ks, k_sem, s, rem(s, SLOTS))

    def start_v(s):
        kv_start(v_ref, vs, v_sem, s, rem(s, SLOTS))

    small = [(x_ref, xv), (ga_ref, gav), (gm_ref, gmv), (cs_ref, csv)]
    small = [pltpu.make_async_copy(a, b, in_sem.at[i]) for i, (a, b) in enumerate(small)]
    wq_into = [ks.at[SLOTS - 1, pl.ds(0, d)], vs.at[SLOTS - 1, pl.ds(0, d)]]
    wq_in = [pltpu.make_async_copy(wq_ref.at[:, pl.ds(i * head, head)], wq_into[i], wq_sem.at[i]) for i in range(heads)]
    wo_in = pltpu.make_async_copy(wo_ref, wov, wo_sem)
    gate_in = [pltpu.make_async_copy(wg_ref.at[:, pl.ds(j * gt, gt)], wgv.at[j], g_sem.at[j]) for j in range(ng)]
    up_in = [pltpu.make_async_copy(wu_ref.at[:, pl.ds(j * gt, gt)], wuv.at[j], u_sem.at[j]) for j in range(ng)]
    down_in = [pltpu.make_async_copy(wd_ref.at[:, pl.ds(j * dt, dt)], wdv.at[j], d_sem.at[j]) for j in range(nd)]
    weights_in = [c for pair in zip(gate_in, up_in) for c in pair] + down_in

    for c in small + wq_in:
        c.start()
    for s in range(SLOTS - 1):
        kv_start(k_ref, ks, k_sem, s, s)
        kv_start(v_ref, vs, v_sem, s, s)
    wo_in.start()

    barrier = pltpu.get_barrier_semaphore()
    for j in range(1, n):
        pl.semaphore_signal(barrier, inc=1, device_id=at(peer(j)), device_id_type=pl.DeviceIdType.MESH)

    for c in small:
        c.wait()
    a = normed(xv[...].astype(F32), gav[...].astype(F32)).astype(BF16)
    cos, sin = csv[0:1], csv[1:2]
    for i in range(heads):
        wq_in[i].wait()
        q = jnp.dot(a, wq_into[i][...], preferred_element_type=F32).astype(BF16).astype(F32)
        lo, hi = q[:, :half], q[:, half:]
        qf[:, i * head : i * head + half] = (lo * cos - hi * sin).astype(BF16).astype(F32)
        qf[:, i * head + half : (i + 1) * head] = (hi * cos + lo * sin).astype(BF16).astype(F32)
    kv_start(k_ref, ks, k_sem, SLOTS - 1, SLOTS - 1)
    kv_start(v_ref, vs, v_sem, SLOTS - 1, SLOTS - 1)
    pl.semaphore_wait(barrier, n - 1)

    def score(s):
        slot = rem(s, SLOTS)
        row = qf[pl.ds(s, 1), :]
        which = lax.broadcasted_iota(jnp.int32, (8, head), 0)
        q = jnp.zeros((8, head), F32)
        for i in range(heads):
            q = jnp.where(which == i, row[:, i * head : (i + 1) * head], q)
        scores[rem(s, 2)] = lax.dot_general(q.astype(BF16), ks[slot], (((1,), (1,)), ((), ())), preferred_element_type=F32)

    def attend(s):
        sc = scores[rem(s, 2)]
        e = jnp.exp((sc - jnp.max(sc, -1, keepdims=True)) * head**-0.5)
        p = (e * (1.0 / jnp.sum(e, -1, keepdims=True))).astype(BF16)
        slot = rem(s, SLOTS)
        hc = cache // 2
        o = jnp.dot(p[:, :hc], vs[slot, :hc], preferred_element_type=F32)
        o = o + jnp.dot(p[:, hc:], vs[slot, hc:], preferred_element_type=F32)
        r = rem(s, block)
        for i in range(heads):
            seen[pl.ds(r, 1), i * head : (i + 1) * head] = o[i : i + 1]

    def term_copy(c, j):
        return pltpu.make_async_remote_copy(
            src_ref=terms.at[0, c],
            dst_ref=terms.at[j, c],
            send_sem=t_send.at[c, j],
            recv_sem=t_recv.at[c, j],
            device_id=at(peer(j)),
            device_id_type=pl.DeviceIdType.MESH,
        )

    def send_terms(c):
        terms[0, c] = jnp.dot(seen[...].astype(BF16), wov[...], preferred_element_type=F32).astype(BF16)
        for j in range(1, n):
            term_copy(c, j).start()

    def take_terms(c):
        for j in range(1, n):
            term_copy(c, j).wait_recv()
        at_rows = tile_at(c, block)
        total = terms[rem(me + n, n), c].astype(F32)
        for r in range(1, n):
            total = total + terms[rem(me - r + n, n), c].astype(F32)
        h = (hf[at_rows, :] + total).astype(BF16).astype(F32)
        hf[at_rows, :] = h
        bf[at_rows, :] = normed(h, gmv[...].astype(F32))

    hf[...] = xv[...].astype(F32)
    kv_wait(k_ref, ks, k_sem, 0)
    score(0)
    first_spare = rows - 1 - SLOTS

    def step(s, _):
        kv_wait(k_ref, ks, k_sem, rem(s + 1, SLOTS))
        kv_wait(v_ref, vs, v_sem, rem(s, SLOTS))
        score(s + 1)
        attend(s)

        @pl.when(s + 1 + SLOTS < rows)
        def _():
            start_k(s + 1 + SLOTS)

        @pl.when(s + SLOTS < rows)
        def _():
            start_v(s + SLOTS)

        for i in range(SLOTS):

            @pl.when(s == first_spare + i)
            def _():
                for c in weights_in[i * 3 : i * 3 + 3]:
                    c.start()

        @pl.when(rem(s, block) == block - 1)
        def _():
            c = s // block

            @pl.when(c == 0)
            def _():
                wo_in.wait()

            send_terms(c)

            @pl.when(c > 0)
            def _():
                take_terms(c - 1)

        return 0

    start_k(SLOTS)
    lax.fori_loop(0, rows - 1, step, 0)
    for c in weights_in[3 * SLOTS :]:
        c.start()
    kv_wait(v_ref, vs, v_sem, (rows - 1) % SLOTS)
    attend(rows - 1)
    last = rows // block - 1
    send_terms(last)
    take_terms(last - 1)
    take_terms(last)

    b16[...] = bf[...].astype(BF16)

    def hidden(j, _):
        pltpu.make_async_copy(wg_ref.at[:, pl.ds(0, gt)], wgv.at[j], g_sem.at[j]).wait()
        pltpu.make_async_copy(wu_ref.at[:, pl.ds(0, gt)], wuv.at[j], u_sem.at[j]).wait()
        gate = jnp.dot(b16[...], wgv[j], preferred_element_type=F32)
        up = jnp.dot(b16[...], wuv[j], preferred_element_type=F32)
        hid[:, tile_at(j, gt)] = (jax.nn.silu(gate) * up).astype(BF16)
        return 0

    lax.fori_loop(0, ng, hidden, 0)

    my_rows = tile_at(me, block)

    def sum_copy(t, j):
        return pltpu.make_async_remote_copy(
            src_ref=out16.at[t, peer(j)],
            dst_ref=sums.at[j, t],
            send_sem=s_send.at[t, j],
            recv_sem=s_recv.at[t, j],
            device_id=at(peer(j)),
            device_id_type=pl.DeviceIdType.MESH,
        )

    def y_at(t, dev):
        return y_ref.at[tile_at(dev, block), tile_at(t, dt)]

    def y_copy(t, j):
        return pltpu.make_async_remote_copy(
            src_ref=yown.at[t],
            dst_ref=y_at(t, me),
            send_sem=y_send.at[t, j],
            recv_sem=y_recv.at[t, j],
            device_id=at(peer(j)),
            device_id_type=pl.DeviceIdType.MESH,
        )

    def y_local(t):
        return pltpu.make_async_copy(yown.at[t], y_at(t, me), own_sem.at[t])

    def finish(t):
        for j in range(1, n):
            sum_copy(t, j).wait_recv()
        total = outf[t, my_rows, :]
        for j in range(1, n):
            total = total + sums[j, t].astype(F32)
        yown[t] = (hf[my_rows, tile_at(t, dt)] + total).astype(BF16)
        for j in range(1, n):
            y_copy(t, j).start()
        y_local(t).start()

    def down(t, _):
        pltpu.make_async_copy(wd_ref.at[:, pl.ds(0, dt)], wdv.at[t], d_sem.at[t]).wait()
        out = jnp.dot(hid[...], wdv[t], preferred_element_type=F32)
        outf[t] = out
        out16[t] = out.reshape(n, block, dt).astype(BF16)
        for j in range(1, n):
            sum_copy(t, j).start()

        @pl.when(t > 1)
        def _():
            finish(t - 2)

        return 0

    lax.fori_loop(0, nd, down, 0)
    finish(nd - 2)
    finish(nd - 1)

    def drain_y(t, _):
        for j in range(1, n):
            sum_copy(t, j).wait_send()
            y_copy(t, j).wait_send()
            y_copy(t, j).wait_recv()
        y_local(t).wait()
        return 0

    def drain_t(c, _):
        for j in range(1, n):
            term_copy(c, j).wait_send()
        return 0

    lax.fori_loop(0, last + 1, drain_t, 0)
    lax.fori_loop(0, nd, drain_y, 0)


def solution(mesh):
    n = mesh.shape["tp"]

    def step(x, k_cache, v_cache, gain_a, wq, wo, gain_m, w_gate, w_up, w_down):
        rows, d = x.shape
        cache, _, head = k_cache.shape[1:]
        half = head // 2
        angle = F32(cache - 1) * THETA ** (-jnp.arange(half, dtype=F32) / half)
        turn = jnp.stack([jnp.cos(angle), jnp.sin(angle)])
        block = rows // n
        chunks = rows // block
        ff = w_gate.shape[1]
        ng, nd = ff // HIDDEN_TILE, d // OUT_TILE
        k, v = (c.reshape(rows, cache, head) for c in (k_cache, v_cache))
        dma = pltpu.SemaphoreType.DMA
        return pl.pallas_call(
            functools.partial(layer, n),
            out_shape=jax.ShapeDtypeStruct((rows, d), BF16),
            in_specs=[pl.BlockSpec(memory_space=pl.ANY)] * 11,
            out_specs=pl.BlockSpec(memory_space=pl.ANY),
            scratch_shapes=[
                pltpu.VMEM((rows, d), BF16),
                pltpu.VMEM((1, d), BF16),
                pltpu.VMEM((1, d), BF16),
                pltpu.VMEM((2, half), F32),
                pltpu.VMEM((SLOTS, cache, head), BF16),
                pltpu.VMEM((SLOTS, cache, head), BF16),
                pltpu.VMEM(wo.shape, BF16),
                pltpu.VMEM((ng, d, HIDDEN_TILE), BF16),
                pltpu.VMEM((ng, d, HIDDEN_TILE), BF16),
                pltpu.VMEM((nd, ff, OUT_TILE), BF16),
                pltpu.VMEM((rows, wq.shape[1]), F32),
                pltpu.VMEM((2, 8, cache), F32),
                pltpu.VMEM((block, wq.shape[1]), F32),
                pltpu.VMEM((n, chunks, block, d), BF16),
                pltpu.VMEM((rows, d), F32),
                pltpu.VMEM((rows, d), F32),
                pltpu.VMEM((rows, d), BF16),
                pltpu.VMEM((rows, ff), BF16),
                pltpu.VMEM((nd, rows, OUT_TILE), F32),
                pltpu.VMEM((nd, n, block, OUT_TILE), BF16),
                pltpu.VMEM((n, nd, block, OUT_TILE), BF16),
                pltpu.VMEM((nd, block, OUT_TILE), BF16),
                dma((4,)),
                dma((SLOTS,)),
                dma((SLOTS,)),
                dma((2,)),
                dma,
                dma((ng,)),
                dma((ng,)),
                dma((nd,)),
                dma((chunks, n)),
                dma((chunks, n)),
                dma((nd, n)),
                dma((nd, n)),
                dma((nd, n)),
                dma((nd, n)),
                dma((nd,)),
            ],
            compiler_params=pltpu.CompilerParams(collective_id=0, has_side_effects=True, vmem_limit_bytes=VMEM_LIMIT),
        )(x, k, v, gain_a.reshape(1, d), wq, wo, gain_m.reshape(1, d), w_gate, w_up, w_down, turn)

    states, cache, columns, rows_of = P("dp", None), P("dp", None, "tp", None), P(None, "tp"), P("tp", None)
    return jax.shard_map(
        step,
        mesh=mesh,
        in_specs=(states, cache, cache, P(None), columns, rows_of, P(None), columns, columns, rows_of),
        out_specs=states,
        check_vma=False,
    )
```

```python
import functools

import jax
import jax.numpy as jnp
from jax import lax
from jax.experimental import pallas as pl
from jax.experimental.pallas import tpu as pltpu
from jax.sharding import PartitionSpec as P

HEAD = 256
THETA = 10000
SLOTS = 3
SPLIT = 2
HIDDEN_TILE = 256
OUT_TILE = 512
FEW = 4
LAG = 4
VMEM_LIMIT = 66_000_000
F32 = jnp.float32
BF16 = jnp.bfloat16


def rem(a, b):
    return a % b if isinstance(a, int) else lax.rem(a, b)


def tile_at(i, size):
    return pl.ds(i * size if isinstance(i, int) else pl.multiple_of(i * size, size), size)


def normed(wide, gain):
    scale = lax.rsqrt(jnp.mean(wide * wide, -1, keepdims=True) + 1e-6)
    return wide * scale * gain


def layer(
    n,
    x_ref, k_ref, v_ref, ga_ref, wq_ref, wo_ref, gm_ref, wg_ref, wu_ref, wd_ref, cos_ref, sin_ref,
    y_ref,
    xv, gav, gmv, cosv, sinv, ks, vs, wov, wgv, wuv, wdv, qf, scores, probs, seen, terms, hf, bf, b16, hid, outf, out16, pair, mid, sums,
    in_sem, k_sem, v_sem, wq_sem, wo_sem, g_sem, u_sem, d_sem,
    t_send, t_recv, a_send, a_recv, m_send, m_recv, y_send, y_recv, f_send, f_recv,
):
    me = lax.axis_index("tp")
    rows, d = xv.shape
    cache, head = ks.shape[1:]
    heads = wq_ref.shape[1] // head
    half = head // 2
    few = terms.shape[2]
    block = rows // n
    group = block // few
    ng, nd = wgv.shape[0], wdv.shape[0]
    gt, dt = wgv.shape[2], wdv.shape[2]
    chips = n // 2
    core, chip = lax.rem(me, 2), me // 2
    partner = me + 1 - 2 * core

    def peer(j):
        return lax.rem(me + j, n)

    def chip_at(j):
        return lax.rem(chip + j, chips)

    def remote(src, dst, send, recv, dev):
        return pltpu.make_async_remote_copy(
            src_ref=src, dst_ref=dst, send_sem=send, recv_sem=recv, device_id={"tp": dev}, device_id_type=pl.DeviceIdType.MESH
        )

    def kv_start(hbm, slots, sem, s, slot):
        part = cache // SPLIT
        for i in range(SPLIT):
            pltpu.make_async_copy(hbm.at[s, pl.ds(i * part, part)], slots.at[slot, pl.ds(i * part, part)], sem.at[slot]).start()

    def kv_wait(hbm, slots, sem, slot):
        pltpu.make_async_copy(hbm.at[0], slots.at[slot], sem.at[slot]).wait()

    def start_k(s):
        kv_start(k_ref, ks, k_sem, s, rem(s, SLOTS))

    def start_v(s):
        kv_start(v_ref, vs, v_sem, s, rem(s, SLOTS))

    small = [(x_ref, xv), (ga_ref, gav), (gm_ref, gmv), (cos_ref, cosv), (sin_ref, sinv)]
    small = [pltpu.make_async_copy(a, b, in_sem.at[i]) for i, (a, b) in enumerate(small)]
    wq_into = [ks.at[SLOTS - 1, pl.ds(0, d)], vs.at[SLOTS - 1, pl.ds(0, d)]]
    wq_in = [pltpu.make_async_copy(wq_ref.at[:, pl.ds(i * head, head)], wq_into[i], wq_sem.at[i]) for i in range(heads)]
    wo_in = pltpu.make_async_copy(wo_ref, wov, wo_sem)
    gate_in = [pltpu.make_async_copy(wg_ref.at[:, pl.ds(j * gt, gt)], wgv.at[j], g_sem.at[j]) for j in range(ng)]
    up_in = [pltpu.make_async_copy(wu_ref.at[:, pl.ds(j * gt, gt)], wuv.at[j], u_sem.at[j]) for j in range(ng)]
    down_in = [pltpu.make_async_copy(wd_ref.at[:, pl.ds(j * dt, dt)], wdv.at[j], d_sem.at[j]) for j in range(nd)]
    weights_in = [c for two in zip(gate_in, up_in) for c in two] + down_in

    for c in small + wq_in:
        c.start()
    for s in range(SLOTS - 1):
        start_k(s)
        start_v(s)
    wo_in.start()

    barrier = pltpu.get_barrier_semaphore()
    for j in range(1, n):
        pl.semaphore_signal(barrier, inc=1, device_id={"tp": peer(j)}, device_id_type=pl.DeviceIdType.MESH)

    for c in small:
        c.wait()
    a = normed(xv[...].astype(F32), gav[...].astype(F32).reshape(1, d)).astype(BF16)
    cos, sin = cosv[...], sinv[...]
    for i in range(heads):
        wq_in[i].wait()
        q = jnp.dot(a, wq_into[i][...], preferred_element_type=F32).astype(BF16).astype(F32)
        lo, hi = q[:, :half], q[:, half:]
        qf[:, i * head : i * head + half] = (lo * cos - hi * sin).astype(BF16).astype(F32)
        qf[:, i * head + half : (i + 1) * head] = (hi * cos + lo * sin).astype(BF16).astype(F32)
    start_k(SLOTS - 1)
    start_v(SLOTS - 1)
    hf[...] = xv[...].astype(F32)
    pl.semaphore_wait(barrier, n - 1)

    def score(s):
        row = qf[pl.ds(s, 1), :]
        which = lax.broadcasted_iota(jnp.int32, (8, head), 0)
        q = jnp.zeros((8, head), F32)
        for i in range(heads):
            q = jnp.where(which == i, row[:, i * head : (i + 1) * head], q)
        scores[rem(s, 2)] = lax.dot_general(
            q.astype(BF16), ks[rem(s, SLOTS)], (((1,), (1,)), ((), ())), preferred_element_type=F32
        )

    def soften(s):
        sc = scores[rem(s, 2)]
        e = jnp.exp((sc - jnp.max(sc, -1, keepdims=True)) * head**-0.5)
        probs[rem(s, 2)] = (e * (1.0 / jnp.sum(e, -1, keepdims=True))).astype(BF16)

    def gather(s):
        p, slot, hc = probs[rem(s, 2)], rem(s, SLOTS), cache // 2
        o = jnp.dot(p[:, :hc], vs[slot, :hc], preferred_element_type=F32)
        o = o + jnp.dot(p[:, hc:], vs[slot, hc:], preferred_element_type=F32)
        for i in range(heads):
            seen[pl.ds(rem(s, few), 1), i * head : (i + 1) * head] = o[i : i + 1]

    def term_copy(c, j):
        return remote(terms.at[0, c], terms.at[j, c], t_send.at[c, j], t_recv.at[c, j], peer(j))

    def send_terms(c):
        terms[0, c] = jnp.dot(seen[...].astype(BF16), wov[...], preferred_element_type=F32)[:few].astype(BF16)
        for j in range(1, n):
            term_copy(c, j).start()

    def take_terms(g):
        totals = []
        for i in range(group):
            c = g * group + i
            for j in range(1, n):
                term_copy(c, j).wait_recv()
            total = terms[lax.rem(me, n), c].astype(F32)
            for r in range(1, n):
                total = total + terms[lax.rem(me - r + n, n), c].astype(F32)
            totals.append(total)
        at_rows = tile_at(g, block)
        h = (hf[at_rows, :] + jnp.concatenate(totals, 0)).astype(BF16).astype(F32)
        hf[at_rows, :] = h
        bf[at_rows, :] = normed(h, gmv[...].astype(F32).reshape(1, d))

    kv_wait(k_ref, ks, k_sem, 0)
    score(0)
    start_k(SLOTS)
    kv_wait(k_ref, ks, k_sem, 1)
    score(1)
    start_k(SLOTS + 1)
    soften(0)
    first_spare = rows - 1 - SLOTS

    def step(s, _):
        kv_wait(k_ref, ks, k_sem, rem(s + 1, SLOTS))
        kv_wait(v_ref, vs, v_sem, rem(s - 1, SLOTS))
        gather(s - 1)
        soften(s)
        score(s + 1)

        @pl.when(s + 1 + SLOTS < rows)
        def _():
            start_k(s + 1 + SLOTS)

        @pl.when(s - 1 + SLOTS < rows)
        def _():
            start_v(s - 1 + SLOTS)

        for i in range(SLOTS):

            @pl.when(s == first_spare + i)
            def _():
                for c in weights_in[i * 3 : i * 3 + 3]:
                    c.start()

        @pl.when(lax.rem(s, few) == 0)
        def _():
            c = s // few - 1

            @pl.when(c == 0)
            def _():
                wo_in.wait()

            send_terms(c)
            g = s // block - 1

            @pl.when((lax.rem(s, block) == 0) & (g > 0))
            def _():
                take_terms(g - 1)

        return 0

    lax.fori_loop(1, rows - 1, step, 0)
    for c in weights_in[3 * SLOTS :]:
        c.start()
    kv_wait(v_ref, vs, v_sem, (rows - 2) % SLOTS)
    soften(rows - 1)
    gather(rows - 2)
    kv_wait(v_ref, vs, v_sem, (rows - 1) % SLOTS)
    gather(rows - 1)
    last = rows // few - 1
    send_terms(last)
    take_terms(n - 2)
    take_terms(n - 1)

    b16[...] = bf[...].astype(BF16)

    def hidden(j, _):
        pltpu.make_async_copy(wg_ref.at[:, pl.ds(0, gt)], wgv.at[j], g_sem.at[j]).wait()
        pltpu.make_async_copy(wu_ref.at[:, pl.ds(0, gt)], wuv.at[j], u_sem.at[j]).wait()
        gate = jnp.dot(b16[...], wgv[j], preferred_element_type=F32)
        up = jnp.dot(b16[...], wuv[j], preferred_element_type=F32)
        hid[:, tile_at(j, gt)] = (jax.nn.silu(gate) * up).astype(BF16)
        return 0

    lax.fori_loop(0, ng, hidden, 0)

    def a_copy(t):
        return remote(out16.at[t, 1 - core], pair.at[t], a_send.at[t], a_recv.at[t], partner)

    def m_copy(t, j):
        to = chip_at(j)
        return remote(mid.at[t, to], sums.at[j, t], m_send.at[t, j], m_recv.at[t, j], 2 * to + core)

    def y_at(t, dev):
        return y_ref.at[tile_at(dev, block), tile_at(t, dt)]

    def y_copy(t, j):
        mine = y_at(t, me)
        return remote(mine, mine, y_send.at[t, j], y_recv.at[t, j], partner if j == 0 else 2 * chip_at(j) + core)

    def f_copy(t, j):
        theirs = y_at(t, 2 * chip_at(chips - j) + core)
        return remote(theirs, theirs, f_send.at[t, j], f_recv.at[t, j], partner)

    def multiply(t):
        pltpu.make_async_copy(wd_ref.at[:, pl.ds(0, dt)], wdv.at[t], d_sem.at[t]).wait()
        out = jnp.dot(hid[...], wdv[t], preferred_element_type=F32)
        outf[t] = out
        out = out.astype(BF16)
        for i in range(n):
            out16[t, i % 2, i // 2] = out[i * block : (i + 1) * block]
        a_copy(t).start()

    def add_pair(t):
        a_copy(t).wait_recv()
        for j in range(1, chips):
            to = chip_at(j)
            mid[t, to] = (outf[t, tile_at(2 * to + core, block), :] + pair[t, to].astype(F32)).astype(BF16)
        for j in range(1, chips):
            m_copy(t, j).start()

    def finish(t):
        total = outf[t, tile_at(me, block), :] + pair[t, chip].astype(F32)
        for j in range(1, chips):
            m_copy(t, j).wait_recv()
        for j in range(1, chips):
            total = total + sums[j, t].astype(F32)
        y_ref[tile_at(me, block), tile_at(t, dt)] = (hf[tile_at(me, block), tile_at(t, dt)] + total).astype(BF16)
        for j in range(chips):
            y_copy(t, j).start()

    def forward(t):
        for j in range(1, chips):
            y_copy(t, j).wait_recv()
            f_copy(t, j).start()

    def down(u, _):
        pl.when(u < nd)(lambda: multiply(u))
        for lag, then in ((1, add_pair), (LAG, finish), (2 * LAG, forward)):
            pl.when((u >= lag) & (u < nd + lag))(lambda: then(u - lag))
        return 0

    lax.fori_loop(0, nd + 2 * LAG, down, 0)

    def drain_y(t, _):
        a_copy(t).wait_send()
        for j in range(chips):
            y_copy(t, j).wait_send()
        y_copy(t, 0).wait_recv()
        for j in range(1, chips):
            m_copy(t, j).wait_send()
            f_copy(t, j).wait_send()
            f_copy(t, j).wait_recv()
        return 0

    def drain_t(c, _):
        for j in range(1, n):
            term_copy(c, j).wait_send()
        return 0

    lax.fori_loop(0, last + 1, drain_t, 0)
    lax.fori_loop(0, nd, drain_y, 0)


def solution(mesh):
    n = mesh.shape["tp"]

    def step(x, k_cache, v_cache, gain_a, wq, wo, gain_m, w_gate, w_up, w_down):
        rows, d = x.shape
        cache, _, head = k_cache.shape[1:]
        half = head // 2
        angle = F32(cache - 1) * THETA ** (-jnp.arange(half, dtype=F32)[None] / half)
        block = rows // n
        chunks = rows // FEW
        ff = w_gate.shape[1]
        ng, nd = ff // HIDDEN_TILE, d // OUT_TILE
        k, v = (c.reshape(rows, cache, head) for c in (k_cache, v_cache))
        dma = pltpu.SemaphoreType.DMA
        return pl.pallas_call(
            functools.partial(layer, n),
            out_shape=jax.ShapeDtypeStruct((rows, d), BF16),
            in_specs=[pl.BlockSpec(memory_space=pl.ANY)] * 12,
            out_specs=pl.BlockSpec(memory_space=pltpu.VMEM),
            scratch_shapes=[
                pltpu.VMEM((rows, d), BF16),
                pltpu.VMEM((d,), BF16),
                pltpu.VMEM((d,), BF16),
                pltpu.VMEM((1, half), F32),
                pltpu.VMEM((1, half), F32),
                pltpu.VMEM((SLOTS, cache, head), BF16),
                pltpu.VMEM((SLOTS, cache, head), BF16),
                pltpu.VMEM(wo.shape, BF16),
                pltpu.VMEM((ng, d, HIDDEN_TILE), BF16),
                pltpu.VMEM((ng, d, HIDDEN_TILE), BF16),
                pltpu.VMEM((nd, ff, OUT_TILE), BF16),
                pltpu.VMEM((rows, wq.shape[1]), F32),
                pltpu.VMEM((2, 8, cache), F32),
                pltpu.VMEM((2, 8, cache), BF16),
                pltpu.VMEM((8, wq.shape[1]), F32),
                pltpu.VMEM((n, chunks, FEW, d), BF16),
                pltpu.VMEM((rows, d), F32),
                pltpu.VMEM((rows, d), F32),
                pltpu.VMEM((rows, d), BF16),
                pltpu.VMEM((rows, ff), BF16),
                pltpu.VMEM((nd, rows, OUT_TILE), F32),
                pltpu.VMEM((nd, 2, n // 2, block, OUT_TILE), BF16),
                pltpu.VMEM((nd, n // 2, block, OUT_TILE), BF16),
                pltpu.VMEM((nd, n // 2, block, OUT_TILE), BF16),
                pltpu.VMEM((n // 2, nd, block, OUT_TILE), BF16),
                dma((5,)),
                dma((SLOTS,)),
                dma((SLOTS,)),
                dma((2,)),
                dma,
                dma((ng,)),
                dma((ng,)),
                dma((nd,)),
                dma((chunks, n)),
                dma((chunks, n)),
                dma((nd,)),
                dma((nd,)),
                dma((nd, n // 2)),
                dma((nd, n // 2)),
                dma((nd, n // 2)),
                dma((nd, n // 2)),
                dma((nd, n // 2)),
                dma((nd, n // 2)),
            ],
            compiler_params=pltpu.CompilerParams(collective_id=0, has_side_effects=True, vmem_limit_bytes=VMEM_LIMIT),
        )(x, k, v, gain_a, wq, wo, gain_m, w_gate, w_up, w_down, jnp.cos(angle), jnp.sin(angle))

    states, cache, columns, rows_of = P("dp", None), P("dp", None, "tp", None), P(None, "tp"), P("tp", None)
    return jax.shard_map(
        step,
        mesh=mesh,
        in_specs=(states, cache, cache, P(None), columns, rows_of, P(None), columns, columns, rows_of),
        out_specs=states,
        check_vma=False,
    )
```

```python
import functools

import jax
import jax.numpy as jnp
from jax import lax
from jax.experimental import pallas as pl
from jax.experimental.pallas import tpu as pltpu
from jax.sharding import PartitionSpec as P

HEAD = 256
THETA = 10000
SLOTS = 3
SPLIT = 2
HIDDEN_TILE = 256
OUT_TILE = 512
FEW = 4
LAG = 3
AHEAD = 6
EARLY = 8
VMEM_LIMIT = 66_000_000
F32 = jnp.float32
BF16 = jnp.bfloat16


def rem(a, b):
    return a % b if isinstance(a, int) else lax.rem(a, b)


def tile_at(i, size):
    return pl.ds(i * size if isinstance(i, int) else pl.multiple_of(i * size, size), size)


def normed(wide, gain):
    scale = lax.rsqrt(jnp.mean(wide * wide, -1, keepdims=True) + 1e-6)
    return wide * scale * gain


def layer(
    n,
    x_ref, k_ref, v_ref, ga_ref, wq_ref, wo_ref, gm_ref, wg_ref, wu_ref, wd_ref, cos_ref, sin_ref,
    y_ref,
    xv, gav, gmv, cosv, sinv, ks, vs, wov, wgv, wuv, wdv, qf, scores, probs, seen, terms, hf, bf, b16, hid, outf, out16, pair, mid, sums,
    in_sem, k_sem, v_sem, wq_sem, wo_sem, g_sem, u_sem, d_sem,
    t_send, t_recv, a_send, a_recv, m_send, m_recv, y_send, y_recv, f_send, f_recv,
):
    me = lax.axis_index("tp")
    rows, d = xv.shape
    cache, head = ks.shape[1:]
    heads = wq_ref.shape[1] // head
    half = head // 2
    few = terms.shape[2]
    block = rows // n
    group = block // few
    ng, nd = wgv.shape[0], wdv.shape[0]
    gt, dt = wgv.shape[2], wdv.shape[2]
    chips = n // 2
    core, chip = lax.rem(me, 2), me // 2
    partner = me + 1 - 2 * core

    def peer(j):
        return lax.rem(me + j, n)

    def chip_at(j):
        return lax.rem(chip + j, chips)

    def remote(src, dst, send, recv, dev):
        return pltpu.make_async_remote_copy(
            src_ref=src, dst_ref=dst, send_sem=send, recv_sem=recv, device_id={"tp": dev}, device_id_type=pl.DeviceIdType.MESH
        )

    def kv_start(hbm, slots, sem, s, slot):
        part = cache // SPLIT
        for i in range(SPLIT):
            pltpu.make_async_copy(hbm.at[s, pl.ds(i * part, part)], slots.at[slot, pl.ds(i * part, part)], sem.at[slot]).start()

    def kv_wait(hbm, slots, sem, slot):
        pltpu.make_async_copy(hbm.at[0], slots.at[slot], sem.at[slot]).wait()

    def start_k(s):
        kv_start(k_ref, ks, k_sem, s, rem(s, SLOTS))

    def start_v(s):
        kv_start(v_ref, vs, v_sem, s, rem(s, SLOTS))

    small = [(x_ref, xv), (ga_ref, gav), (gm_ref, gmv), (cos_ref, cosv), (sin_ref, sinv)]
    small = [pltpu.make_async_copy(a, b, in_sem.at[i]) for i, (a, b) in enumerate(small)]
    wq_into = [ks.at[SLOTS - 1, pl.ds(0, d)], vs.at[SLOTS - 1, pl.ds(0, d)]]
    wq_in = [pltpu.make_async_copy(wq_ref.at[:, pl.ds(i * head, head)], wq_into[i], wq_sem.at[i]) for i in range(heads)]
    wo_in = pltpu.make_async_copy(wo_ref, wov, wo_sem)
    gate_in = [pltpu.make_async_copy(wg_ref.at[:, pl.ds(j * gt, gt)], wgv.at[j], g_sem.at[j]) for j in range(ng)]
    up_in = [pltpu.make_async_copy(wu_ref.at[:, pl.ds(j * gt, gt)], wuv.at[j], u_sem.at[j]) for j in range(ng)]
    down_in = [pltpu.make_async_copy(wd_ref.at[:, pl.ds(j * dt, dt)], wdv.at[j], d_sem.at[j]) for j in range(nd)]
    weights_in = [c for two in zip(gate_in, up_in) for c in two] + down_in

    for c in small + wq_in:
        c.start()
    for s in range(SLOTS - 1):
        start_k(s)
        start_v(s)
    wo_in.start()

    barrier = pltpu.get_barrier_semaphore()
    for j in range(1, n):
        pl.semaphore_signal(barrier, inc=1, device_id={"tp": peer(j)}, device_id_type=pl.DeviceIdType.MESH)

    for c in small:
        c.wait()
    a = normed(xv[...].astype(F32), gav[...].astype(F32).reshape(1, d)).astype(BF16)
    cos, sin = cosv[...], sinv[...]
    for i in range(heads):
        wq_in[i].wait()
        q = jnp.dot(a, wq_into[i][...], preferred_element_type=F32).astype(BF16).astype(F32)
        lo, hi = q[:, :half], q[:, half:]
        qf[:, i * head : i * head + half] = (lo * cos - hi * sin).astype(BF16).astype(F32)
        qf[:, i * head + half : (i + 1) * head] = (hi * cos + lo * sin).astype(BF16).astype(F32)
    start_k(SLOTS - 1)
    start_v(SLOTS - 1)
    hf[...] = xv[...].astype(F32)
    pl.semaphore_wait(barrier, n - 1)

    def score(s):
        row = qf[pl.ds(s, 1), :]
        which = lax.broadcasted_iota(jnp.int32, (8, head), 0)
        q = jnp.zeros((8, head), F32)
        for i in range(heads):
            q = jnp.where(which == i, row[:, i * head : (i + 1) * head], q)
        scores[rem(s, 2)] = lax.dot_general(
            q.astype(BF16), ks[rem(s, SLOTS)], (((1,), (1,)), ((), ())), preferred_element_type=F32
        )

    def soften(s):
        sc = scores[rem(s, 2)]
        e = jnp.exp((sc - jnp.max(sc, -1, keepdims=True)) * head**-0.5)
        probs[rem(s, 2)] = (e * (1.0 / jnp.sum(e, -1, keepdims=True))).astype(BF16)

    def gather(s):
        p, slot, hc = probs[rem(s, 2)], rem(s, SLOTS), cache // 2
        o = jnp.dot(p[:, :hc], vs[slot, :hc], preferred_element_type=F32)
        o = o + jnp.dot(p[:, hc:], vs[slot, hc:], preferred_element_type=F32)
        for i in range(heads):
            seen[pl.ds(rem(s, few), 1), i * head : (i + 1) * head] = o[i : i + 1]

    def term_copy(c, j):
        return remote(terms.at[0, c], terms.at[j, c], t_send.at[c, j], t_recv.at[c, j], peer(j))

    def send_terms(c):
        terms[0, c] = jnp.dot(seen[...].astype(BF16), wov[...], preferred_element_type=F32)[:few].astype(BF16)
        for j in range(1, n):
            term_copy(c, j).start()

    def take_terms(g):
        totals = []
        for i in range(group):
            c = g * group + i
            for j in range(1, n):
                term_copy(c, j).wait_recv()
            total = terms[lax.rem(me, n), c].astype(F32)
            for r in range(1, n):
                total = total + terms[lax.rem(me - r + n, n), c].astype(F32)
            totals.append(total)
        at_rows = tile_at(g, block)
        h = (hf[at_rows, :] + jnp.concatenate(totals, 0)).astype(BF16).astype(F32)
        hf[at_rows, :] = h
        bf[at_rows, :] = normed(h, gmv[...].astype(F32).reshape(1, d))

    kv_wait(k_ref, ks, k_sem, 0)
    score(0)
    start_k(SLOTS)
    kv_wait(k_ref, ks, k_sem, 1)
    score(1)
    start_k(SLOTS + 1)
    soften(0)
    first_spare = rows - 1 - SLOTS

    def step(s, _):
        kv_wait(k_ref, ks, k_sem, rem(s + 1, SLOTS))
        kv_wait(v_ref, vs, v_sem, rem(s - 1, SLOTS))
        gather(s - 1)
        soften(s)
        score(s + 1)

        @pl.when(s + 1 + SLOTS < rows)
        def _():
            start_k(s + 1 + SLOTS)

        @pl.when(s - 1 + SLOTS < rows)
        def _():
            start_v(s - 1 + SLOTS)

        for i in range(SLOTS):

            @pl.when(s == first_spare + i)
            def _():
                weights_in[i].start()

        @pl.when(lax.rem(s, few) == 0)
        def _():
            c = s // few - 1

            @pl.when(c == 0)
            def _():
                wo_in.wait()

            send_terms(c)
            g = s // block - 1

            @pl.when((lax.rem(s, block) == 0) & (g > 0))
            def _():
                take_terms(g - 1)

        return 0

    lax.fori_loop(1, rows - 1, step, 0)
    for c in weights_in[SLOTS : SLOTS + 2]:
        c.start()
    kv_wait(v_ref, vs, v_sem, (rows - 2) % SLOTS)
    soften(rows - 1)
    gather(rows - 2)
    for c in weights_in[SLOTS + 2 : AHEAD]:
        c.start()
    kv_wait(v_ref, vs, v_sem, (rows - 1) % SLOTS)
    gather(rows - 1)
    last = rows // few - 1
    send_terms(last)
    take_terms(n - 2)
    for i in range(EARLY):
        weights_in[i].wait()
        weights_in[i + AHEAD].start()
    take_terms(n - 1)

    b16[...] = bf[...].astype(BF16)

    def start_down(t):
        pltpu.make_async_copy(wd_ref.at[:, tile_at(t, dt)], wdv.at[t], d_sem.at[t]).start()

    def hidden(j, _):
        @pl.when(j >= EARLY // 2)
        def _():
            pltpu.make_async_copy(wg_ref.at[:, pl.ds(0, gt)], wgv.at[j], g_sem.at[j]).wait()
            pltpu.make_async_copy(wu_ref.at[:, pl.ds(0, gt)], wuv.at[j], u_sem.at[j]).wait()
            start_down(2 * (j - EARLY // 2))
            start_down(2 * (j - EARLY // 2) + 1)

        gate = jnp.dot(b16[...], wgv[j], preferred_element_type=F32)
        up = jnp.dot(b16[...], wuv[j], preferred_element_type=F32)
        hid[:, tile_at(j, gt)] = (jax.nn.silu(gate) * up).astype(BF16)
        return 0

    assert EARLY + AHEAD == 2 * ng and nd <= 2 * ng
    lax.fori_loop(0, ng, hidden, 0)
    for t in range(AHEAD, nd):
        start_down(t)

    def a_copy(t):
        return remote(out16.at[t, 1 - core], pair.at[t], a_send.at[t], a_recv.at[t], partner)

    def m_copy(t, j):
        to = chip_at(j)
        return remote(mid.at[t, to], sums.at[j, t], m_send.at[t, j], m_recv.at[t, j], 2 * to + core)

    def y_at(t, dev):
        return y_ref.at[tile_at(dev, block), tile_at(t, dt)]

    def y_copy(t, j):
        mine = y_at(t, me)
        return remote(mine, mine, y_send.at[t, j], y_recv.at[t, j], partner if j == 0 else 2 * chip_at(j) + core)

    def f_copy(t, j):
        theirs = y_at(t, 2 * chip_at(chips - j) + core)
        return remote(theirs, theirs, f_send.at[t, j], f_recv.at[t, j], partner)

    def multiply(t):
        pltpu.make_async_copy(wd_ref.at[:, pl.ds(0, dt)], wdv.at[t], d_sem.at[t]).wait()
        out = jnp.dot(hid[...], wdv[t], preferred_element_type=F32)
        outf[t] = out
        out = out.astype(BF16)
        for i in range(n):
            out16[t, i % 2, i // 2] = out[i * block : (i + 1) * block]
        a_copy(t).start()

    def add_pair(t):
        a_copy(t).wait_recv()
        for j in range(1, chips):
            to = chip_at(j)
            mid[t, to] = (outf[t, tile_at(2 * to + core, block), :] + pair[t, to].astype(F32)).astype(BF16)
        for j in range(1, chips):
            m_copy(t, j).start()

    def finish(t):
        total = outf[t, tile_at(me, block), :] + pair[t, chip].astype(F32)
        for j in range(1, chips):
            m_copy(t, j).wait_recv()
        for j in range(1, chips):
            total = total + sums[j, t].astype(F32)
        y_ref[tile_at(me, block), tile_at(t, dt)] = (hf[tile_at(me, block), tile_at(t, dt)] + total).astype(BF16)
        for j in range(chips):
            y_copy(t, j).start()

    def forward(t):
        for j in range(1, chips):
            y_copy(t, j).wait_recv()
            f_copy(t, j).start()

    def down(u, _):
        pl.when(u < nd)(lambda: multiply(u))
        for lag, then in ((LAG, add_pair), (nd + LAG, finish), (2 * nd + LAG, forward)):
            pl.when((u >= lag) & (u < nd + lag))(lambda: then(u - lag))
        return 0

    lax.fori_loop(0, 3 * nd + LAG, down, 0)

    def drain_y(t, _):
        a_copy(t).wait_send()
        for j in range(chips):
            y_copy(t, j).wait_send()
        y_copy(t, 0).wait_recv()
        for j in range(1, chips):
            m_copy(t, j).wait_send()
            f_copy(t, j).wait_send()
            f_copy(t, j).wait_recv()
        return 0

    def drain_t(c, _):
        for j in range(1, n):
            term_copy(c, j).wait_send()
        return 0

    lax.fori_loop(0, last + 1, drain_t, 0)
    lax.fori_loop(0, nd, drain_y, 0)


def solution(mesh):
    n = mesh.shape["tp"]

    def step(x, k_cache, v_cache, gain_a, wq, wo, gain_m, w_gate, w_up, w_down):
        rows, d = x.shape
        cache, _, head = k_cache.shape[1:]
        half = head // 2
        angle = F32(cache - 1) * THETA ** (-jnp.arange(half, dtype=F32)[None] / half)
        block = rows // n
        chunks = rows // FEW
        ff = w_gate.shape[1]
        ng, nd = ff // HIDDEN_TILE, d // OUT_TILE
        k, v = (c.reshape(rows, cache, head) for c in (k_cache, v_cache))
        dma = pltpu.SemaphoreType.DMA
        return pl.pallas_call(
            functools.partial(layer, n),
            out_shape=pltpu.VMEM((rows, d), BF16),
            in_specs=[pl.BlockSpec(memory_space=pl.ANY)] * 12,
            out_specs=pl.BlockSpec(memory_space=pltpu.VMEM),
            scratch_shapes=[
                pltpu.VMEM((rows, d), BF16),
                pltpu.VMEM((d,), BF16),
                pltpu.VMEM((d,), BF16),
                pltpu.VMEM((1, half), F32),
                pltpu.VMEM((1, half), F32),
                pltpu.VMEM((SLOTS, cache, head), BF16),
                pltpu.VMEM((SLOTS, cache, head), BF16),
                pltpu.VMEM(wo.shape, BF16),
                pltpu.VMEM((ng, d, HIDDEN_TILE), BF16),
                pltpu.VMEM((ng, d, HIDDEN_TILE), BF16),
                pltpu.VMEM((nd, ff, OUT_TILE), BF16),
                pltpu.VMEM((rows, wq.shape[1]), F32),
                pltpu.VMEM((2, 8, cache), F32),
                pltpu.VMEM((2, 8, cache), BF16),
                pltpu.VMEM((8, wq.shape[1]), F32),
                pltpu.VMEM((n, chunks, FEW, d), BF16),
                pltpu.VMEM((rows, d), F32),
                pltpu.VMEM((rows, d), F32),
                pltpu.VMEM((rows, d), BF16),
                pltpu.VMEM((rows, ff), BF16),
                pltpu.VMEM((nd, rows, OUT_TILE), F32),
                pltpu.VMEM((nd, 2, n // 2, block, OUT_TILE), BF16),
                pltpu.VMEM((nd, n // 2, block, OUT_TILE), BF16),
                pltpu.VMEM((nd, n // 2, block, OUT_TILE), BF16),
                pltpu.VMEM((n // 2, nd, block, OUT_TILE), BF16),
                dma((5,)),
                dma((SLOTS,)),
                dma((SLOTS,)),
                dma((2,)),
                dma,
                dma((ng,)),
                dma((ng,)),
                dma((nd,)),
                dma((chunks, n)),
                dma((chunks, n)),
                dma((nd,)),
                dma((nd,)),
                dma((nd, n // 2)),
                dma((nd, n // 2)),
                dma((nd, n // 2)),
                dma((nd, n // 2)),
                dma((nd, n // 2)),
                dma((nd, n // 2)),
            ],
            compiler_params=pltpu.CompilerParams(collective_id=0, has_side_effects=True, vmem_limit_bytes=VMEM_LIMIT),
        )(x, k, v, gain_a, wq, wo, gain_m, w_gate, w_up, w_down, jnp.cos(angle), jnp.sin(angle))

    states, cache, columns, rows_of = P("dp", None), P("dp", None, "tp", None), P(None, "tp"), P("tp", None)
    return jax.shard_map(
        step,
        mesh=mesh,
        in_specs=(states, cache, cache, P(None), columns, rows_of, P(None), columns, columns, rows_of),
        out_specs=states,
        check_vma=False,
    )
```
